32 devices in a mesh: dp: 8 (over z, x), tp: 4 (over y, core).
Axes of the slice: x: 2, y: 2, z: 4, core: 2. Of those that a mesh axis runs over, the one named last changes fastest.
Arguments:
- queries: bfloat16 [4096, 8192], P('dp', 'tp'), parts along dimension 0, may hold values from -200 to 200
- new_keys: bfloat16 [4096, 1024], P('dp', 'tp'), parts along dimension 0, may hold values from -9 to 9
- new_values: bfloat16 [4096, 1024], P('dp', 'tp'), parts along dimension 0, may hold values from -60 to 60
- cache_keys: bfloat16 [32, 32768, 128], P('dp', 'tp'), parts along dimension 0, may hold values from -4 to 4
- cache_values: bfloat16 [32, 32768, 128], P('dp', 'tp'), parts along dimension 0, may hold values from -60 to 60
- out_weight: bfloat16 [8192, 8192], P('tp'), may hold values from -0.09375 to 0.09375
- residual: bfloat16 [4096, 8192], P('dp', 'tp'), parts along dimension 0, may hold values from -8 to 8
- norm_gain: bfloat16 [8192], P('tp'), may hold values from 0.5 to 1.5
Outputs:
- normed: bfloat16 [4096, 8192], P('dp', 'tp'), parts along dimension 0
The draws below stay inside these ranges and needn't reach their ends.
There are 8 independent parts, one for each index of `dp`. The reference program is written for one: setup_inputs(seed, part) draws one part's arguments, and reference() takes and returns one part's arrays. A program takes and returns all parts, laid end to end along the dimension named above; an argument that names none is the same for every part. Nothing has to cross between parts.
All inputs are finite; a program needn't handle non-finite values.
Results may differ from the reference program's by a relative error of at most 0.015.
Values may be sent and summed in bfloat16 or wider, within the bound.
A program may use at most 256 MiB of HBM per device.

```python
import math
import jax
import jax.numpy as jnp
from jax import lax

D = 8192
H = 64
KVH = 8
HD = 128
SPAN = 128
SEQS = 4
CTX = 4096
TOK = 512


def build_drawn(key):
    key_stored = jax.random.fold_in(key, 11)
    key_query = jax.random.fold_in(key, 12)
    stored = jax.random.truncated_normal(key_stored, -4.0, 4.0, (SEQS, KVH * CTX, HD), jnp.float32)
    asked = jax.random.truncated_normal(key_query, -4.0, 4.0, (SEQS * SPAN, H * HD), jnp.float32)
    return (stored, asked)


def draw_cache_keys(key, part):
    return build_drawn(key)[0].astype(jnp.bfloat16)


def draw_queries(key, part):
    return build_drawn(key)[1].astype(jnp.bfloat16)


def draw_residual(key, part):
    key_base = jax.random.fold_in(key, 21)
    position = jnp.arange(D, dtype=jnp.float32) / D
    rising = 0.15 * jnp.exp(position * math.log(3.0))
    values = jax.random.truncated_normal(key_base, -4.0, 4.0, (SEQS * SPAN, D), jnp.float32) * rising[None, :]
    return values.astype(jnp.bfloat16)


def spiked(values, own_key, source, target, parts, factor):
    owner, partner = [(jnp.arange(values.shape[dim]) // (values.shape[dim] // parts)).reshape([-1 if axis == dim else 1 for axis in range(values.ndim)]) for dim in (source, target)]
    chosen = jax.random.permutation(own_key, parts)[partner]
    strong = (owner == chosen) | (owner == (partner + parts // 2) % parts)
    return jnp.where(strong, factor * values, values)


def levels(own_key, shape, shards, low, high):
    factor_of = 1.0
    for dim, parts in shards:
        draws = jax.random.uniform(jax.random.fold_in(jax.random.fold_in(own_key, 6), dim), (parts,), jnp.float32, low / len(shards), high / len(shards))
        factor_of = factor_of * jnp.repeat(jnp.exp(draws), shape[dim] // parts).reshape((-1,) + (1,) * (len(shape) - 1 - dim))
    return factor_of


def scatter_about(own_key, shape, deviation, limit, split=(), held_as=jnp.bfloat16):
    drawn = jax.random.normal(own_key, shape, jnp.float32) * deviation
    if len(split) > 0:
        drawn = levels(own_key, shape, split, -0.22, 0.18) * drawn
    return jnp.clip(drawn, min=-limit, max=limit).astype(held_as)


def heavy_noise(stream_key, extent, spread, most, pieces, heavy, held_as=jnp.bfloat16):
    values = spread * jax.random.normal(stream_key, extent, jnp.float32)
    if pieces:
        values = values * levels(stream_key, extent, pieces, -0.22, 0.18)
    return jnp.clip(spiked(values, jax.random.fold_in(stream_key, 3), *heavy), -most, most).astype(held_as)


def setup_inputs(seed: int = 0, part: int = 0) -> dict:
    keys = jax.random.split(jax.random.key(seed), 9)
    part_splits = jax.random.split(jax.random.fold_in(keys[8], part), 9)
    queries = draw_queries(jax.random.fold_in(jax.random.fold_in(keys[8], part), 71), part)
    new_keys = scatter_about(part_splits[1], (TOK, KVH * HD), 1.5, 9.0, ((1, 4),))
    new_values = scatter_about(part_splits[2], (TOK, KVH * HD), 10.0, 60.0, ((1, 4),))
    cache_keys = draw_cache_keys(jax.random.fold_in(jax.random.fold_in(keys[8], part), 71), part)
    cache_values = scatter_about(part_splits[4], (SEQS, KVH * CTX, HD), 10.0, 60.0, ((1, 4),))
    out_weight = heavy_noise(keys[5], (H * HD, D), (H * HD) ** -0.5, 0.09375, ((0, 4),), (0, 1, 4, 2.0))
    residual = draw_residual(jax.random.fold_in(jax.random.fold_in(keys[8], part), 71), part)
    norm_gain = jnp.clip(1.0 + 0.1 * jax.random.normal(keys[7], (D,), jnp.float32), 0.5, 1.5).astype(jnp.bfloat16)
    return {"queries": queries, "new_keys": new_keys, "new_values": new_values, "cache_keys": cache_keys, "cache_values": cache_values, "out_weight": out_weight, "residual": residual, "norm_gain": norm_gain}


def attend_sequence(inputs):
    query_rows, fresh_keys, fresh_values, stored_keys, stored_values = inputs
    groups = H // KVH
    scaling = HD ** (-0.5)
    grouped = query_rows.astype(jnp.float32).reshape(SPAN, KVH, groups, HD)
    old_keys = stored_keys.astype(jnp.float32).reshape(KVH, CTX, HD)
    old_values = stored_values.astype(jnp.float32).reshape(KVH, CTX, HD)
    recent_keys = fresh_keys.astype(jnp.float32).reshape(SPAN, KVH, HD)
    recent_values = fresh_values.astype(jnp.float32).reshape(SPAN, KVH, HD)
    old_scores = jnp.einsum('ighd,gjd->ghij', grouped, old_keys) * scaling
    recent_scores = jnp.einsum('ighd,jgd->ghij', grouped, recent_keys) * scaling
    causal = jnp.arange(SPAN)[:, None] >= jnp.arange(SPAN)[None, :]
    recent_scores = jnp.where(causal, recent_scores, -jnp.inf)
    peak = jnp.maximum(lax.optimization_barrier(jnp.max(old_scores, axis=-1)), lax.optimization_barrier(jnp.max(recent_scores, axis=-1)))
    old_weights = jnp.exp(old_scores - peak[..., None])
    recent_weights = jnp.exp(recent_scores - peak[..., None])
    total = lax.optimization_barrier(jnp.sum(old_weights, axis=-1)) + lax.optimization_barrier(jnp.sum(recent_weights, axis=-1))
    rounded_old = lax.optimization_barrier(old_weights.astype(jnp.bfloat16)).astype(jnp.float32)
    rounded_recent = lax.optimization_barrier(recent_weights.astype(jnp.bfloat16)).astype(jnp.float32)
    mixed = jnp.einsum('ghij,gjd->ighd', rounded_old, old_values)
    mixed = mixed + jnp.einsum('ghij,jgd->ighd', rounded_recent, recent_values)
    result = mixed / jnp.transpose(total, (2, 0, 1))[..., None]
    return result.reshape(SPAN, H * HD).astype(jnp.bfloat16)

def reference(queries, new_keys, new_values, cache_keys, cache_values, out_weight, residual, norm_gain):
    inputs = (queries.reshape(SEQS, SPAN, H * HD), new_keys.reshape(SEQS, SPAN, KVH * HD), new_values.reshape(SEQS, SPAN, KVH * HD), cache_keys, cache_values)
    attended = lax.map(attend_sequence, inputs).reshape(SEQS * SPAN, H * HD)
    projected = jnp.dot(attended, out_weight, preferred_element_type=jnp.float32)
    hidden = residual.astype(jnp.float32) + projected
    power = lax.optimization_barrier(jnp.mean(hidden * hidden, axis=1, keepdims=True))
    normed = hidden * lax.rsqrt(power + 1e-05) * norm_gain.astype(jnp.float32)
    return normed.astype(jnp.bfloat16)
```

```python
import functools

import jax
import jax.numpy as jnp
from jax import lax
from jax.experimental import pallas as pl
from jax.experimental.pallas import tpu as pltpu
from jax.sharding import PartitionSpec as P

D = 8192
KVH = 8
HD = 128
SPAN = 128
SEQS = 4
CTX = 4096


EPSILON = 1e-05


def partner(value, axis, bit):
    mask = 2**bit
    pairs = [(source, source ^ mask) for source in range(lax.axis_size(axis))]
    return lax.ppermute(value, axis, pairs)


def attend_block(query_rows, stored_keys, stored_values, fresh_keys, fresh_values, local_kv):
    heads_here = query_rows.shape[1] // HD
    groups = heads_here // local_kv
    length = stored_keys.shape[1] // local_kv
    scaling = HD ** (-0.5)
    grouped = query_rows.reshape(SEQS, SPAN, local_kv, groups, HD)
    old_keys = stored_keys.reshape(SEQS, local_kv, length, HD)
    old_values = stored_values.reshape(SEQS, local_kv, length, HD)
    scores = (
        jnp.einsum("sighd,sgjd->sghij", grouped, old_keys, preferred_element_type=jnp.float32)
        * scaling
    )
    peak = jnp.max(scores, axis=-1)
    recent_keys = fresh_keys.reshape(SEQS, SPAN, local_kv, HD)
    recent_values = fresh_values.reshape(SEQS, SPAN, local_kv, HD)
    recent_scores = (
        jnp.einsum("sighd,sjgd->sghij", grouped, recent_keys, preferred_element_type=jnp.float32)
        * scaling
    )
    causal = jnp.arange(SPAN)[:, None] >= jnp.arange(SPAN)[None, :]
    recent_scores = jnp.where(causal, recent_scores, -jnp.inf)
    peak = jnp.maximum(peak, jnp.max(recent_scores, axis=-1))
    weights = jnp.exp(scores - peak[..., None])
    total = jnp.sum(weights, axis=-1)
    mixed = jnp.einsum(
        "sghij,sgjd->sighd",
        weights.astype(jnp.bfloat16),
        old_values,
        preferred_element_type=jnp.float32,
    )
    recent_weights = jnp.exp(recent_scores - peak[..., None])
    total = total + jnp.sum(recent_weights, axis=-1)
    mixed = mixed + jnp.einsum(
        "sghij,sjgd->sighd",
        recent_weights.astype(jnp.bfloat16),
        recent_values,
        preferred_element_type=jnp.float32,
    )
    return (mixed, peak, total)


def token_layout(stat):
    return jnp.transpose(stat, (0, 3, 1, 2))[..., None]


def finish_rows(mixed, total):
    result = mixed / token_layout(total)
    return result.reshape(SEQS * SPAN, -1).astype(jnp.bfloat16)


def per_device(
    queries, new_keys, new_values, cache_keys, cache_values, out_weight, residual, norm_gain
):
    tp_size = lax.axis_size("tp")
    paired = tp_size == 2 * KVH
    local_kv = 1 if paired else cache_keys.shape[1] // CTX
    parity = lax.axis_index("tp") % 2

    def join_dims(own_piece, other_piece):
        first = jnp.concatenate([own_piece, other_piece], axis=-1)
        second = jnp.concatenate([other_piece, own_piece], axis=-1)
        return jnp.where(parity == 0, first, second)

    if paired:
        other_keys, other_values, other_stored_keys, other_stored_values = partner(
            (new_keys, new_values, cache_keys, cache_values), "tp", 0
        )
        fresh_keys = join_dims(new_keys, other_keys)
        fresh_values = join_dims(new_values, other_values)
        stored_keys = jnp.concatenate([cache_keys, other_stored_keys], axis=1)
        stored_values = jnp.concatenate([cache_values, other_stored_values], axis=1)
    else:
        fresh_keys, fresh_values = (new_keys, new_values)
        stored_keys, stored_values = (cache_keys, cache_values)
    mixed, peak, total = attend_block(
        queries, stored_keys, stored_values, fresh_keys, fresh_values, local_kv
    )
    attended = finish_rows(mixed, total)
    projected = lax.psum_scatter(
        lax.dot_general(
            out_weight, attended, (((0,), (1,)), ((), ())), preferred_element_type=jnp.float32
        ).astype(jnp.bfloat16),
        "tp",
        scatter_dimension=0,
        tiled=True,
    ).astype(jnp.float32)
    hidden = residual.astype(jnp.float32) + jnp.transpose(projected)
    squares = lax.psum(jnp.sum(hidden * hidden, axis=1), "tp")
    scaled = (
        hidden * lax.rsqrt(squares / D + EPSILON)[:, None] * norm_gain.astype(jnp.float32)[None, :]
    )
    return scaled.astype(jnp.bfloat16)


HEADS_PER_BLOCK = 2
KEY_CHUNK = 1024
CHAINS = 32
PIECES = 4
MASKED = -1e30
LOG2E = 1.4426950408889634
MESH = pl.DeviceIdType.MESH


def attend_step(row, q_ref, k_ref, v_ref, nk_ref, nv_ref, att_ref, vt_ref, qx_ref, slots, column):
    stored = k_ref.shape[1]
    groups = q_ref.shape[1] // HD
    lanes = HEADS_PER_BLOCK * SPAN
    blocks = groups // HEADS_PER_BLOCK
    factor = HD ** (-0.5) * LOG2E
    chunks = [(start, KEY_CHUNK) for start in range(0, stored, KEY_CHUNK)] + [(stored, SPAN)]
    key = lax.broadcasted_iota(jnp.int32, (SPAN, SPAN), 0)
    causal_one = key <= lax.broadcasted_iota(jnp.int32, (SPAN, SPAN), 1)
    causal = jnp.concatenate([causal_one] * HEADS_PER_BLOCK, axis=1)

    def turn_values(start, size):
        values = nv_ref[...] if start == stored else v_ref[0, start : start + size, :]
        vt_ref[:, start : start + size] = jnp.transpose(values)

    def load_queries(block):
        for i in range(HEADS_PER_BLOCK):
            where = (block * HEADS_PER_BLOCK + i) * HD
            scaled = jnp.transpose(q_ref[:, where : where + HD].astype(jnp.float32)) * factor
            high = scaled.astype(jnp.bfloat16)
            low = (scaled - high.astype(jnp.float32)).astype(jnp.bfloat16)
            tokens = slice(i * SPAN, (i + 1) * SPAN)
            qx_ref[block % 2, 0:HD, tokens] = high
            qx_ref[block % 2, HD : 2 * HD, tokens] = low

    def score_chunk(block, start, size, running):
        keys = nk_ref[...] if start == stored else k_ref[0, start : start + size, :]
        tile = jnp.dot(
            jnp.concatenate([keys, keys], axis=1), qx_ref[block % 2],
            preferred_element_type=jnp.float32,
        )
        if start == stored:
            tile = jnp.where(causal, tile, MASKED)
        slots[block % 2][start : start + size, :] = tile
        peak = jnp.max(tile.reshape(size // CHAINS, CHAINS, lanes), axis=0)
        return peak if running is None else jnp.maximum(running, peak)

    def halves(start, size):
        if size < 2 * SPAN:
            return [(start, size)]
        return [(start, size // 2), (start + size // 2, size // 2)]

    def score_halves(block, start, size, running):
        for first, part in halves(start, size):
            running = score_chunk(block, first, part, running)
        return running

    running = None
    load_queries(0)
    for start, size in chunks:
        turn_values(start, size)
        running = score_halves(0, start, size, running)
    for block in range(blocks):
        peak = jnp.max(running, axis=0, keepdims=True)
        running, total, mixed = None, None, [None, None]
        if block + 1 < blocks:
            load_queries(block + 1)
        for start, size in chunks:
            if block + 1 < blocks:
                running = score_halves(block + 1, start, size, running)
            for which, (first, part) in enumerate(halves(start, size)):
                weights = jnp.exp2(slots[block % 2][first : first + part, :] - peak)
                summed = jnp.sum(weights.reshape(part // CHAINS, CHAINS, lanes), axis=0)
                total = summed if total is None else total + summed
                term = jnp.dot(
                    vt_ref[:, first : first + part],
                    weights.astype(jnp.bfloat16),
                    preferred_element_type=jnp.float32,
                )
                mixed[which] = term if mixed[which] is None else mixed[which] + term
        result = (mixed[0] + mixed[1]) * (1.0 / jnp.sum(total, axis=0, keepdims=True))
        for i in range(HEADS_PER_BLOCK):
            where = column + (block * HEADS_PER_BLOCK + i) * HD
            turned = jnp.transpose(result[:, i * SPAN : (i + 1) * SPAN])
            att_ref[pl.ds(row, SPAN), pl.ds(where, HD)] = turned.astype(jnp.bfloat16)


def fused_kernel(
    q_ref, k_ref, v_ref, nk_ref, nv_ref, w_hbm, res_hbm, gain_ref, out_hbm,
    w_ref, att_ref, vt_ref, qx_ref, score_a, score_b, res_ref,
    s1_send, s1_recv, s2_send, s2_recv, own_send, own_recv, sq_send, sq_recv,
    w_sem, res_sem, s1_ss, s1_rs, s2_ss, s2_rs, own_ss, own_rs, sq_ss, sq_rs, out_sem,
):
    s, g = pl.program_id(0), pl.program_id(1)
    parts, local_kv = pl.num_programs(0), pl.num_programs(1)
    width = res_ref.shape[1]
    piece = width // PIECES
    block = score_a.shape[1]
    everyone = SEQS * SPAN
    me = lax.axis_index("tp")
    chip, core = me // 2, me % 2
    sibling = chip * 2 + (1 - core)
    across = (1 - chip) * 2 + core
    diagonal = (1 - chip) * 2 + (1 - core)

    owners = (diagonal, across, sibling, me)

    def w_place(which, j):
        return pl.ds(which % 3 * width + j * piece, piece)

    def w_copy(which, j):
        col = pl.ds(pl.multiple_of(owners[which] * width + j * piece, 128), piece)
        return pltpu.make_async_copy(
            w_hbm.at[:, col], w_ref.at[:, w_place(which, j)], w_sem.at[which * PIECES + j]
        )

    def res_copy():
        return pltpu.make_async_copy(res_hbm, res_ref, res_sem.at[0])

    def remote(src, dst, ss, rs, device):
        return pltpu.make_async_remote_copy(
            src_ref=src, dst_ref=dst, send_sem=ss, recv_sem=rs,
            device_id={"tp": device}, device_id_type=MESH,
        )

    def stage1(p, j):
        col = pl.ds(j * piece, piece)
        return remote(
            s1_send.at[p % 2, :, col], s1_recv.at[p % 2, :, col],
            s1_ss.at[p % 2, j], s1_rs.at[p % 2, j], sibling,
        )

    def stage2(p, j):
        at = (pl.ds(pl.multiple_of(p * SPAN, SPAN), SPAN), pl.ds(j * piece, piece))
        return remote(s2_send.at[at], s2_recv.at[at], s2_ss.at[p, j], s2_rs.at[p, j], across)

    def own(j):
        col = pl.ds(j * piece, piece)
        return remote(own_send.at[:, col], own_recv.at[:, col], own_ss.at[j], own_rs.at[j], sibling)

    def squares(p):
        return [
            remote(sq_send.at[p], sq_recv.at[p, i], sq_ss.at[p, i], sq_rs.at[p, i], device)
            for i, device in enumerate((sibling, across, diagonal))
        ]

    def out_copy(p):
        rows = pl.ds(p * SPAN, SPAN)
        return pltpu.make_async_copy(att_ref.at[rows], out_hbm.at[rows], out_sem.at[p])

    @pl.when((s == 0) & (g == 0))
    def _():
        barrier = pltpu.get_barrier_semaphore()
        for device in (sibling, across, diagonal):
            pl.semaphore_signal(barrier, inc=1, device_id={"tp": device}, device_id_type=MESH)
        for which in range(2):
            for j in range(PIECES):
                w_copy(which, j).start()
        pl.semaphore_wait(barrier, 3)

    @pl.when((s == 1) & (g == 0))
    def _():
        for j in range(PIECES):
            w_copy(2, j).start()
        res_copy().start()

    attend_step(
        pl.multiple_of(s * SPAN, SPAN),
        q_ref, k_ref, v_ref, nk_ref, nv_ref, att_ref, vt_ref, qx_ref, (score_a, score_b),
        pl.multiple_of(g * q_ref.shape[1], 128),
    )

    def project(rows, which, j):
        return jnp.dot(
            att_ref[rows, :], w_ref[:, w_place(which, j)], preferred_element_type=jnp.float32
        )

    @pl.when(g == local_kv - 1)
    def _():
        rows = pl.ds(pl.multiple_of(s * SPAN, SPAN), SPAN)

        @pl.when(s == 0)
        def _():
            for which in range(2):
                for j in range(PIECES):
                    w_copy(which, j).wait()

        @pl.when(s > 1)
        def _():
            for j in range(PIECES):
                stage1(s - 2, j).wait_send()

        for j in range(PIECES):
            s1_send[s % 2, :, j * piece : (j + 1) * piece] = project(rows, 0, j).astype(
                jnp.bfloat16
            )
            stage1(s, j).start()

        @pl.when(s == parts - 1)
        def _():
            for j in range(PIECES):
                w_copy(3, j).start()

        for j in range(PIECES):
            near = project(rows, 1, j)
            stage1(s, j).wait_recv()
            col = slice(j * piece, (j + 1) * piece)
            both = near + s1_recv[s % 2, :, col].astype(jnp.float32)
            s2_send[rows, col] = both.astype(jnp.bfloat16)
            stage2(s, j).start()

    def held(p, start):
        first = (start // block) * everyone + p * SPAN
        return (slice(first, first + SPAN), slice(start % block, start % block + 128))

    def collect(p):
        for j in range(PIECES):
            stage2(p, j).wait()
        rows = slice(p * SPAN, (p + 1) * SPAN)
        lanes = None
        for start in range(0, width, 128):
            col = slice(start, start + 128)
            value = (
                score_a[held(p, start)]
                + own_recv[rows, col].astype(jnp.float32)
                + s2_recv[rows, col].astype(jnp.float32)
            )
            score_a[held(p, start)] = value
            lanes = value * value if lanes is None else lanes + value * value
        row = jnp.sum(jnp.transpose(lanes), axis=0, keepdims=True)
        sq_send[p] = jnp.broadcast_to(row, (8, SPAN))
        for copy in squares(p):
            copy.start()

    def finish(p):
        for copy in squares(p):
            copy.wait()
        summed = sq_send[p] + sq_recv[p, 0] + sq_recv[p, 1] + sq_recv[p, 2]
        power = jnp.transpose(jnp.broadcast_to(summed[0:1, :], (SPAN, SPAN))) / D
        scale = lax.rsqrt(power + EPSILON)
        for start in range(0, width, 128):
            gain = gain_ref[:, start : start + 128].astype(jnp.float32)
            scaled = score_a[held(p, start)] * scale * gain
            att_ref[p * SPAN : (p + 1) * SPAN, start : start + 128] = scaled.astype(jnp.bfloat16)
        out_copy(p).start()

    @pl.when((s == parts - 1) & (g == local_kv - 1))
    def _():
        for j in range(PIECES):
            w_copy(2, j).wait()
        res_copy().wait()
        for j in range(PIECES):
            own_send[:, j * piece : (j + 1) * piece] = project(slice(None), 2, j).astype(
                jnp.bfloat16
            )
            own(j).start()
        for j in range(PIECES):
            w_copy(3, j).wait()
        for j in range(PIECES):
            result = project(slice(None), 3, j)
            for start in range(0, piece, block):
                first = (j * piece + start) // block * everyone
                score_a[first : first + everyone, :] = result[:, start : start + block] + res_ref[
                    :, j * piece + start : j * piece + start + block
                ].astype(jnp.float32)
        for j in range(PIECES):
            own(j).wait()
        for p in range(SEQS - 1):
            collect(p)
        for p in range(SEQS - 1):
            finish(p)
        collect(SEQS - 1)
        finish(SEQS - 1)
        for p in (SEQS - 2, SEQS - 1):
            for j in range(PIECES):
                stage1(p, j).wait_send()
        for p in range(SEQS):
            out_copy(p).wait()


def fused(queries, new_keys, new_values, cache_keys, cache_values, out_weight, residual, norm_gain):
    length = cache_keys.shape[1] // (new_keys.shape[1] // HD)
    local_kv = new_keys.shape[1] // HD
    group_width = queries.shape[1] // local_kv
    tokens, width = residual.shape
    keys_all = length + SPAN
    lanes = HEADS_PER_BLOCK * SPAN
    bf16, f32 = jnp.bfloat16, jnp.float32
    dma = pltpu.SemaphoreType.DMA
    return pl.pallas_call(
        fused_kernel,
        grid=(SEQS, local_kv),
        out_shape=jax.ShapeDtypeStruct(residual.shape, bf16),
        in_specs=[
            pl.BlockSpec((SPAN, group_width), lambda s, g: (s, g)),
            pl.BlockSpec((1, length, HD), lambda s, g: (s, g, 0)),
            pl.BlockSpec((1, length, HD), lambda s, g: (s, g, 0)),
            pl.BlockSpec((SPAN, HD), lambda s, g: (s, g)),
            pl.BlockSpec((SPAN, HD), lambda s, g: (s, g)),
            pl.BlockSpec(memory_space=pl.ANY),
            pl.BlockSpec(memory_space=pl.ANY),
            pl.BlockSpec((1, width), lambda s, g: (0, 0)),
        ],
        out_specs=pl.BlockSpec(memory_space=pl.ANY),
        scratch_shapes=[
            pltpu.VMEM((out_weight.shape[0], 3 * width), bf16),
            pltpu.VMEM((tokens, queries.shape[1]), bf16),
            pltpu.VMEM((HD, keys_all), bf16),
            pltpu.VMEM((2, lanes, 2 * HD), bf16),
            pltpu.VMEM((keys_all, lanes), f32),
            pltpu.VMEM((keys_all, lanes), f32),
            pltpu.VMEM((tokens, width), bf16),
            pltpu.VMEM((2, SPAN, width), bf16),
            pltpu.VMEM((2, SPAN, width), bf16),
            pltpu.VMEM((tokens, width), bf16),
            pltpu.VMEM((tokens, width), bf16),
            pltpu.VMEM((tokens, width), bf16),
            pltpu.VMEM((tokens, width), bf16),
            pltpu.VMEM((SEQS, 8, SPAN), f32),
            pltpu.VMEM((SEQS, 3, 8, SPAN), f32),
            dma((4 * PIECES,)),
            dma((1,)),
            dma((2, PIECES)),
            dma((2, PIECES)),
            dma((SEQS, PIECES)),
            dma((SEQS, PIECES)),
            dma((PIECES,)),
            dma((PIECES,)),
            dma((SEQS, 3)),
            dma((SEQS, 3)),
            dma((SEQS,)),
        ],
        compiler_params=pltpu.CompilerParams(
            collective_id=0,
            has_side_effects=True,
            vmem_limit_bytes=67043328,
            dimension_semantics=("arbitrary", "arbitrary"),
        ),
    )(
        queries, cache_keys, cache_values, new_keys, new_values, out_weight, residual,
        norm_gain.reshape(1, -1),
    )


def solution(mesh):
    in_specs = (
        P("dp", "tp"),
        P("dp", "tp"),
        P("dp", "tp"),
        P("dp", "tp", None),
        P("dp", "tp", None),
        P("tp", None),
        P("dp", "tp"),
        P("tp"),
    )
    out_specs = P("dp", "tp")
    return jax.shard_map(
        fused if mesh.shape["tp"] == 4 else per_device, mesh=mesh, in_specs=in_specs, out_specs=out_specs, check_vma=False
    )
```

```python
import functools

import jax
import jax.numpy as jnp
from jax import lax
from jax.experimental import pallas as pl
from jax.experimental.pallas import tpu as pltpu
from jax.sharding import PartitionSpec as P

D = 8192
KVH = 8
HD = 128
SPAN = 128
SEQS = 4
CTX = 4096


EPSILON = 1e-05


def partner(value, axis, bit):
    mask = 2**bit
    pairs = [(source, source ^ mask) for source in range(lax.axis_size(axis))]
    return lax.ppermute(value, axis, pairs)


def attend_block(query_rows, stored_keys, stored_values, fresh_keys, fresh_values, local_kv):
    heads_here = query_rows.shape[1] // HD
    groups = heads_here // local_kv
    length = stored_keys.shape[1] // local_kv
    scaling = HD ** (-0.5)
    grouped = query_rows.reshape(SEQS, SPAN, local_kv, groups, HD)
    old_keys = stored_keys.reshape(SEQS, local_kv, length, HD)
    old_values = stored_values.reshape(SEQS, local_kv, length, HD)
    scores = (
        jnp.einsum("sighd,sgjd->sghij", grouped, old_keys, preferred_element_type=jnp.float32)
        * scaling
    )
    peak = jnp.max(scores, axis=-1)
    recent_keys = fresh_keys.reshape(SEQS, SPAN, local_kv, HD)
    recent_values = fresh_values.reshape(SEQS, SPAN, local_kv, HD)
    recent_scores = (
        jnp.einsum("sighd,sjgd->sghij", grouped, recent_keys, preferred_element_type=jnp.float32)
        * scaling
    )
    causal = jnp.arange(SPAN)[:, None] >= jnp.arange(SPAN)[None, :]
    recent_scores = jnp.where(causal, recent_scores, -jnp.inf)
    peak = jnp.maximum(peak, jnp.max(recent_scores, axis=-1))
    weights = jnp.exp(scores - peak[..., None])
    total = jnp.sum(weights, axis=-1)
    mixed = jnp.einsum(
        "sghij,sgjd->sighd",
        weights.astype(jnp.bfloat16),
        old_values,
        preferred_element_type=jnp.float32,
    )
    recent_weights = jnp.exp(recent_scores - peak[..., None])
    total = total + jnp.sum(recent_weights, axis=-1)
    mixed = mixed + jnp.einsum(
        "sghij,sjgd->sighd",
        recent_weights.astype(jnp.bfloat16),
        recent_values,
        preferred_element_type=jnp.float32,
    )
    return (mixed, peak, total)


def token_layout(stat):
    return jnp.transpose(stat, (0, 3, 1, 2))[..., None]


def finish_rows(mixed, total):
    result = mixed / token_layout(total)
    return result.reshape(SEQS * SPAN, -1).astype(jnp.bfloat16)


def per_device(
    queries, new_keys, new_values, cache_keys, cache_values, out_weight, residual, norm_gain
):
    tp_size = lax.axis_size("tp")
    paired = tp_size == 2 * KVH
    local_kv = 1 if paired else cache_keys.shape[1] // CTX
    parity = lax.axis_index("tp") % 2

    def join_dims(own_piece, other_piece):
        first = jnp.concatenate([own_piece, other_piece], axis=-1)
        second = jnp.concatenate([other_piece, own_piece], axis=-1)
        return jnp.where(parity == 0, first, second)

    if paired:
        other_keys, other_values, other_stored_keys, other_stored_values = partner(
            (new_keys, new_values, cache_keys, cache_values), "tp", 0
        )
        fresh_keys = join_dims(new_keys, other_keys)
        fresh_values = join_dims(new_values, other_values)
        stored_keys = jnp.concatenate([cache_keys, other_stored_keys], axis=1)
        stored_values = jnp.concatenate([cache_values, other_stored_values], axis=1)
    else:
        fresh_keys, fresh_values = (new_keys, new_values)
        stored_keys, stored_values = (cache_keys, cache_values)
    mixed, peak, total = attend_block(
        queries, stored_keys, stored_values, fresh_keys, fresh_values, local_kv
    )
    attended = finish_rows(mixed, total)
    projected = lax.psum_scatter(
        lax.dot_general(
            out_weight, attended, (((0,), (1,)), ((), ())), preferred_element_type=jnp.float32
        ).astype(jnp.bfloat16),
        "tp",
        scatter_dimension=0,
        tiled=True,
    ).astype(jnp.float32)
    hidden = residual.astype(jnp.float32) + jnp.transpose(projected)
    squares = lax.psum(jnp.sum(hidden * hidden, axis=1), "tp")
    scaled = (
        hidden * lax.rsqrt(squares / D + EPSILON)[:, None] * norm_gain.astype(jnp.float32)[None, :]
    )
    return scaled.astype(jnp.bfloat16)


HEADS_PER_BLOCK = 2
KEY_CHUNK = 1024
CHAINS = 32
PIECES = 4
MASKED = -1e30
LOG2E = 1.4426950408889634
MESH = pl.DeviceIdType.MESH


def attend_step(row, q_ref, k_ref, v_ref, nk_ref, nv_ref, att_ref, vt_ref, qx_ref, slots, column):
    stored = k_ref.shape[1]
    groups = q_ref.shape[1] // HD
    lanes = HEADS_PER_BLOCK * SPAN
    blocks = groups // HEADS_PER_BLOCK
    factor = HD ** (-0.5) * LOG2E
    chunks = [(start, KEY_CHUNK) for start in range(0, stored, KEY_CHUNK)] + [(stored, SPAN)]
    key = lax.broadcasted_iota(jnp.int32, (SPAN, SPAN), 0)
    causal_one = key <= lax.broadcasted_iota(jnp.int32, (SPAN, SPAN), 1)
    causal = jnp.concatenate([causal_one] * HEADS_PER_BLOCK, axis=1)

    def turn_values(start, size):
        values = nv_ref[...] if start == stored else v_ref[0, start : start + size, :]
        vt_ref[:, start : start + size] = jnp.transpose(values)

    def load_queries(block):
        for i in range(HEADS_PER_BLOCK):
            where = (block * HEADS_PER_BLOCK + i) * HD
            scaled = jnp.transpose(q_ref[:, where : where + HD].astype(jnp.float32)) * factor
            high = scaled.astype(jnp.bfloat16)
            low = (scaled - high.astype(jnp.float32)).astype(jnp.bfloat16)
            tokens = slice(i * SPAN, (i + 1) * SPAN)
            qx_ref[block % 2, 0:HD, tokens] = high
            qx_ref[block % 2, HD : 2 * HD, tokens] = low

    def score_chunk(block, start, size, running):
        keys = nk_ref[...] if start == stored else k_ref[0, start : start + size, :]
        tile = jnp.dot(
            jnp.concatenate([keys, keys], axis=1), qx_ref[block % 2],
            preferred_element_type=jnp.float32,
        )
        if start == stored:
            tile = jnp.where(causal, tile, MASKED)
        slots[block % 2][start : start + size, :] = tile
        peak = jnp.max(tile.reshape(size // CHAINS, CHAINS, lanes), axis=0)
        return peak if running is None else jnp.maximum(running, peak)

    def halves(start, size):
        if size < 2 * SPAN:
            return [(start, size)]
        return [(start, size // 2), (start + size // 2, size // 2)]

    def score_halves(block, start, size, running):
        for first, part in halves(start, size):
            running = score_chunk(block, first, part, running)
        return running

    running = None
    load_queries(0)
    for start, size in chunks:
        turn_values(start, size)
        running = score_halves(0, start, size, running)
    for block in range(blocks):
        peak = jnp.max(running, axis=0, keepdims=True)
        running, total, mixed = None, None, [None, None]
        if block + 1 < blocks:
            load_queries(block + 1)
        for start, size in chunks:
            if block + 1 < blocks:
                running = score_halves(block + 1, start, size, running)
            for which, (first, part) in enumerate(halves(start, size)):
                weights = jnp.exp2(slots[block % 2][first : first + part, :] - peak)
                summed = jnp.sum(weights.reshape(part // CHAINS, CHAINS, lanes), axis=0)
                total = summed if total is None else total + summed
                term = jnp.dot(
                    vt_ref[:, first : first + part],
                    weights.astype(jnp.bfloat16),
                    preferred_element_type=jnp.float32,
                )
                mixed[which] = term if mixed[which] is None else mixed[which] + term
        result = (mixed[0] + mixed[1]) * (1.0 / jnp.sum(total, axis=0, keepdims=True))
        for i in range(HEADS_PER_BLOCK):
            where = column + (block * HEADS_PER_BLOCK + i) * HD
            turned = jnp.transpose(result[:, i * SPAN : (i + 1) * SPAN])
            att_ref[pl.ds(row, SPAN), pl.ds(where, HD)] = turned.astype(jnp.bfloat16)


def fused_kernel(
    q_ref, k_ref, v_ref, nk_ref, nv_ref, w_hbm, res_hbm, gain_ref, out_hbm,
    w_ref, att_ref, vt_ref, qx_ref, score_a, score_b, res_ref, near_ref,
    s1_send, s1_recv, s2_send, s2_recv, own_send, own_recv, sq_send, sq_recv,
    w_sem, res_sem, s1_ss, s1_rs, s2_ss, s2_rs, own_ss, own_rs, sq_ss, sq_rs, out_sem,
):
    s, g = pl.program_id(0), pl.program_id(1)
    parts, local_kv = pl.num_programs(0), pl.num_programs(1)
    width = res_ref.shape[1]
    piece = width // PIECES
    block = score_a.shape[1]
    everyone = SEQS * SPAN
    me = lax.axis_index("tp")
    chip, core = me // 2, me % 2
    sibling = chip * 2 + (1 - core)
    across = (1 - chip) * 2 + core
    diagonal = (1 - chip) * 2 + (1 - core)

    owners = (diagonal, across, sibling, me)

    def w_place(which, j):
        return pl.ds(which % 3 * width + j * piece, piece)

    def w_copy(which, j):
        col = pl.ds(pl.multiple_of(owners[which] * width + j * piece, 128), piece)
        return pltpu.make_async_copy(
            w_hbm.at[:, col], w_ref.at[:, w_place(which, j)], w_sem.at[which * PIECES + j]
        )

    def res_copy():
        return pltpu.make_async_copy(res_hbm, res_ref, res_sem.at[0])

    def remote(src, dst, ss, rs, device):
        return pltpu.make_async_remote_copy(
            src_ref=src, dst_ref=dst, send_sem=ss, recv_sem=rs,
            device_id={"tp": device}, device_id_type=MESH,
        )

    def stage1(p, j):
        col = pl.ds(j * piece, piece)
        return remote(
            s1_send.at[p % 2, :, col], s1_recv.at[p % 2, :, col],
            s1_ss.at[p % 2, j], s1_rs.at[p % 2, j], sibling,
        )

    def stage2(p, j):
        at = (pl.ds(pl.multiple_of(p * SPAN, SPAN), SPAN), pl.ds(j * piece, piece))
        return remote(s2_send.at[at], s2_recv.at[at], s2_ss.at[p, j], s2_rs.at[p, j], across)

    def own(j):
        col = pl.ds(j * piece, piece)
        return remote(own_send.at[:, col], own_recv.at[:, col], own_ss.at[j], own_rs.at[j], sibling)

    def squares(p):
        return [
            remote(sq_send.at[p], sq_recv.at[p, i], sq_ss.at[p, i], sq_rs.at[p, i], device)
            for i, device in enumerate((sibling, across, diagonal))
        ]

    def out_copy(p):
        rows = pl.ds(p * SPAN, SPAN)
        return pltpu.make_async_copy(att_ref.at[rows], out_hbm.at[rows], out_sem.at[p])

    @pl.when((s == 0) & (g == 0))
    def _():
        barrier = pltpu.get_barrier_semaphore()
        for device in (sibling, across, diagonal):
            pl.semaphore_signal(barrier, inc=1, device_id={"tp": device}, device_id_type=MESH)
        for which in range(2):
            for j in range(PIECES):
                w_copy(which, j).start()
        pl.semaphore_wait(barrier, 3)

    @pl.when((s == 1) & (g == 0))
    def _():
        for j in range(PIECES):
            w_copy(2, j).start()
        res_copy().start()

    attend_step(
        pl.multiple_of(s * SPAN, SPAN),
        q_ref, k_ref, v_ref, nk_ref, nv_ref, att_ref, vt_ref, qx_ref, (score_a, score_b),
        pl.multiple_of(g * q_ref.shape[1], 128),
    )

    def project(rows, which, j):
        return jnp.dot(
            att_ref[rows, :], w_ref[:, w_place(which, j)], preferred_element_type=jnp.float32
        )

    @pl.when(g == local_kv - 1)
    def _():
        rows = pl.ds(pl.multiple_of(s * SPAN, SPAN), SPAN)

        @pl.when(s == 0)
        def _():
            for which in range(2):
                for j in range(PIECES):
                    w_copy(which, j).wait()

        @pl.when(s > 1)
        def _():
            for j in range(PIECES):
                stage1(s - 2, j).wait_send()

        for j in range(PIECES):
            s1_send[s % 2, :, j * piece : (j + 1) * piece] = project(rows, 0, j).astype(
                jnp.bfloat16
            )
            stage1(s, j).start()
        for j in range(PIECES):
            near_ref[:, j * piece : (j + 1) * piece] = project(rows, 1, j)
        for j in range(PIECES):
            stage1(s, j).wait_recv()
            col = slice(j * piece, (j + 1) * piece)
            both = near_ref[:, col] + s1_recv[s % 2, :, col].astype(jnp.float32)
            s2_send[rows, col] = both.astype(jnp.bfloat16)
            stage2(s, j).start()

    def held(p, start):
        first = (start // block) * everyone + p * SPAN
        return (slice(first, first + SPAN), slice(start % block, start % block + 128))

    def collect(p):
        for j in range(PIECES):
            stage2(p, j).wait()
        rows = slice(p * SPAN, (p + 1) * SPAN)
        lanes = None
        for start in range(0, width, 128):
            col = slice(start, start + 128)
            value = (
                score_a[held(p, start)]
                + own_recv[rows, col].astype(jnp.float32)
                + s2_recv[rows, col].astype(jnp.float32)
            )
            score_a[held(p, start)] = value
            lanes = value * value if lanes is None else lanes + value * value
        row = jnp.sum(jnp.transpose(lanes), axis=0, keepdims=True)
        sq_send[p] = jnp.broadcast_to(row, (8, SPAN))
        for copy in squares(p):
            copy.start()

    def finish(p):
        for copy in squares(p):
            copy.wait()
        summed = sq_send[p] + sq_recv[p, 0] + sq_recv[p, 1] + sq_recv[p, 2]
        power = jnp.transpose(jnp.broadcast_to(summed[0:1, :], (SPAN, SPAN))) / D
        scale = lax.rsqrt(power + EPSILON)
        for start in range(0, width, 128):
            gain = gain_ref[start : start + 128].astype(jnp.float32)[None, :]
            scaled = score_a[held(p, start)] * scale * gain
            att_ref[p * SPAN : (p + 1) * SPAN, start : start + 128] = scaled.astype(jnp.bfloat16)
        out_copy(p).start()

    @pl.when((s == parts - 1) & (g == local_kv - 1))
    def _():
        for j in range(PIECES):
            w_copy(3, j).start()
        for j in range(PIECES):
            w_copy(2, j).wait()
        res_copy().wait()
        for j in range(PIECES):
            own_send[:, j * piece : (j + 1) * piece] = project(slice(None), 2, j).astype(
                jnp.bfloat16
            )
            own(j).start()
        for j in range(PIECES):
            w_copy(3, j).wait()
        for j in range(PIECES):
            result = project(slice(None), 3, j)
            for start in range(0, piece, block):
                first = (j * piece + start) // block * everyone
                score_a[first : first + everyone, :] = result[:, start : start + block] + res_ref[
                    :, j * piece + start : j * piece + start + block
                ].astype(jnp.float32)
        for j in range(PIECES):
            own(j).wait()
        for p in range(SEQS):
            collect(p)
        for p in range(SEQS):
            finish(p)
        for p in (SEQS - 2, SEQS - 1):
            for j in range(PIECES):
                stage1(p, j).wait_send()
        for p in range(SEQS):
            out_copy(p).wait()


def hand_over(in_hbm, out_hbm, held, in_sem, out_sem):
    rows = held.shape[1]

    def copies(i):
        span = pl.ds(i * rows, rows)
        return (
            pltpu.make_async_copy(in_hbm.at[span], held.at[i], in_sem.at[i]),
            pltpu.make_async_copy(held.at[i], out_hbm.at[span], out_sem.at[i]),
        )

    for i in range(SEQS):
        copies(i)[0].start()
    for i in range(SEQS):
        copies(i)[0].wait()
        copies(i)[1].start()
    for i in range(SEQS):
        copies(i)[1].wait()


def fused(queries, new_keys, new_values, cache_keys, cache_values, out_weight, residual, norm_gain):
    length = cache_keys.shape[1] // (new_keys.shape[1] // HD)
    local_kv = new_keys.shape[1] // HD
    group_width = queries.shape[1] // local_kv
    tokens, width = residual.shape
    keys_all = length + SPAN
    lanes = HEADS_PER_BLOCK * SPAN
    bf16, f32 = jnp.bfloat16, jnp.float32
    dma = pltpu.SemaphoreType.DMA
    result = pl.pallas_call(
        fused_kernel,
        grid=(SEQS, local_kv),
        out_shape=jax.ShapeDtypeStruct(residual.shape, bf16),
        in_specs=[
            pl.BlockSpec((SPAN, group_width), lambda s, g: (s, g)),
            pl.BlockSpec((1, length, HD), lambda s, g: (s, g, 0)),
            pl.BlockSpec((1, length, HD), lambda s, g: (s, g, 0)),
            pl.BlockSpec((SPAN, HD), lambda s, g: (s, g)),
            pl.BlockSpec((SPAN, HD), lambda s, g: (s, g)),
            pl.BlockSpec(memory_space=pl.ANY),
            pl.BlockSpec(memory_space=pl.ANY),
            pl.BlockSpec((width,), lambda s, g: (0,)),
        ],
        out_specs=pl.BlockSpec(memory_space=pl.ANY),
        scratch_shapes=[
            pltpu.VMEM((out_weight.shape[0], 3 * width), bf16),
            pltpu.VMEM((tokens, queries.shape[1]), bf16),
            pltpu.VMEM((HD, keys_all), bf16),
            pltpu.VMEM((2, lanes, 2 * HD), bf16),
            pltpu.VMEM((keys_all, lanes), f32),
            pltpu.VMEM((keys_all, lanes), f32),
            pltpu.VMEM((tokens, width), bf16),
            pltpu.VMEM((SPAN, width), f32),
            pltpu.VMEM((2, SPAN, width), bf16),
            pltpu.VMEM((2, SPAN, width), bf16),
            pltpu.VMEM((tokens, width), bf16),
            pltpu.VMEM((tokens, width), bf16),
            pltpu.VMEM((tokens, width), bf16),
            pltpu.VMEM((tokens, width), bf16),
            pltpu.VMEM((SEQS, 8, SPAN), f32),
            pltpu.VMEM((SEQS, 3, 8, SPAN), f32),
            dma((4 * PIECES,)),
            dma((1,)),
            dma((2, PIECES)),
            dma((2, PIECES)),
            dma((SEQS, PIECES)),
            dma((SEQS, PIECES)),
            dma((PIECES,)),
            dma((PIECES,)),
            dma((SEQS, 3)),
            dma((SEQS, 3)),
            dma((SEQS,)),
        ],
        compiler_params=pltpu.CompilerParams(
            collective_id=0,
            has_side_effects=True,
            vmem_limit_bytes=67043328,
            dimension_semantics=("arbitrary", "arbitrary"),
        ),
    )(
        queries, cache_keys, cache_values, new_keys, new_values, out_weight, residual,
        norm_gain,
    )
    return pl.pallas_call(
        hand_over,
        out_shape=jax.ShapeDtypeStruct(result.shape, bf16),
        in_specs=[pl.BlockSpec(memory_space=pl.ANY)],
        out_specs=pl.BlockSpec(memory_space=pl.ANY),
        scratch_shapes=[
            pltpu.VMEM((SEQS, tokens // SEQS, width), bf16), dma((SEQS,)), dma((SEQS,)),
        ],
    )(result)


def solution(mesh):
    in_specs = (
        P("dp", "tp"),
        P("dp", "tp"),
        P("dp", "tp"),
        P("dp", "tp", None),
        P("dp", "tp", None),
        P("tp", None),
        P("dp", "tp"),
        P("tp"),
    )
    out_specs = P("dp", "tp")
    return jax.shard_map(
        fused if mesh.shape["tp"] == 4 else per_device, mesh=mesh, in_specs=in_specs, out_specs=out_specs, check_vma=False
    )
```
